32 devices in a mesh: member: 2 (over y), lat: 4 (over z), lon: 4 (over x, core).
Axes of the slice: x: 2, y: 2, z: 4, core: 2. Of those that a mesh axis runs over, the one named last changes fastest.
Arguments:
- layer_inputs: bfloat16 [2, 256, 192, 512], P('member', None, 'lat', 'lon'), may hold values from -6 to 6
- conv_weight: bfloat16 [3, 3, 69, 256], replicated, may hold values from -0.125 to 0.125
- channel_offset: float32 [69], replicated, may hold values from -4 to 4
- observed: bfloat16 [69, 192, 512], P(None, 'lat', 'lon'), may hold values from -6 to 6
- var_weight: float32 [69], replicated, may hold values from 0.5 to 4
Outputs:
- predicted_fields: bfloat16 [2, 69, 192, 512], P('member', None, 'lat', 'lon')
- input_slope_field: bfloat16 [2, 256, 192, 512], P('member', None, 'lat', 'lon')
The draws below stay inside these ranges and needn't reach their ends.
All inputs are finite; a program needn't handle non-finite values.
Results may differ from the reference program's by a relative error of at most 0.0063.
Values may be sent and summed in bfloat16 or wider, within the bound.
A program may use at most 192 MiB of HBM per device.

```python
import math
import jax
import jax.numpy as jnp
from jax import lax

C = 256
OV = 69
MEMBERS = 2
NLAT = 192
NLON = 512


def steps_of(key, dims, cuts, low, top_value):
    def one(axis_at, shards_of):
        heights = jax.random.uniform(jax.random.fold_in(jax.random.fold_in(key, 6), axis_at), (shards_of,), jnp.float32, low / len(cuts), top_value / len(cuts))
        return jnp.repeat(jnp.exp(heights), dims[axis_at] // shards_of).reshape((-1,) + (1,) * (len(dims) - axis_at - 1))

    loudness = one(*cuts[0])
    for cut in cuts[1:]:
        loudness = loudness * one(*cut)
    return loudness


def gaussian(rng, extent, scale, bound, shards=(), kind=jnp.bfloat16):
    array = jax.random.normal(rng, extent, jnp.float32) * scale
    if len(shards) > 0:
        array = steps_of(rng, extent, shards, -0.22, 0.18) * array
    return jnp.clip(array, min=-bound, max=bound).astype(kind)


def setup_inputs(seed: int = 0) -> dict:
    streams_of = jax.random.split(jax.random.key(seed), 6)
    layer_inputs = gaussian(streams_of[0], (MEMBERS, C, NLAT, NLON), 1.0, 6.0, ((0, 2), (2, 4), (3, 4)))
    conv_weight = gaussian(streams_of[1], (3, 3, OV, C), (9 * C) ** -0.5, 0.125)
    channel_offset = gaussian(streams_of[2], (OV,), 1.0, 4.0, (), jnp.float32)
    observed = gaussian(streams_of[3], (OV, NLAT, NLON), 1.0, 6.0, ((1, 4), (2, 4)))
    var_weight = jnp.clip(jnp.exp(jax.random.uniform(streams_of[4], (OV,), jnp.float32, math.log(0.5), math.log(4.0))), 0.5, 4.0)
    return {"layer_inputs": layer_inputs, "conv_weight": conv_weight, "channel_offset": channel_offset, "observed": observed, "var_weight": var_weight}


smoothing = 0.25

def smooth(difference):
    return difference * lax.rsqrt(difference * difference + smoothing * smoothing)

def cycle_pad(field):
    widened = jnp.concatenate([field[..., -1:], field, field[..., :1]], axis=-1)
    zeros = jnp.zeros_like(widened[..., :1, :])
    return jnp.concatenate([zeros, widened, zeros], axis=-2)

def reference(layer_inputs, conv_weight, channel_offset, observed, var_weight):

    def apply_output_layer(member_features):
        padded = cycle_pad(member_features)
        accumulated_outcome = jnp.zeros((OV, NLAT * NLON), jnp.float32)
        for row_tap in range(3):
            for col_tap in range(3):
                window = padded[:, row_tap:row_tap + NLAT, col_tap:col_tap + NLON].reshape(C, NLAT * NLON)
                accumulated_outcome = accumulated_outcome + jnp.dot(conv_weight[row_tap, col_tap], window, preferred_element_type=jnp.float32)
        return (accumulated_outcome.reshape(OV, NLAT, NLON) + channel_offset[:, None, None]).astype(jnp.bfloat16)
    predicted_fields = lax.map(apply_output_layer, layer_inputs)
    quantity_table = predicted_fields.astype(jnp.float32)

    def add_member(running, member_values):
        return (running + smooth(quantity_table - member_values[None]), None)
    pair_sums, unused = lax.scan(add_member, jnp.zeros_like(quantity_table), quantity_table)
    row_index = jnp.arange(NLAT).astype(jnp.float32)
    lat_weight = jnp.cos((-80.0 + 160.0 * (row_index + 0.5) / NLAT) * (jnp.pi / 180.0))
    target = observed.astype(jnp.float32)[None]
    gradient = (lat_weight[:, None] * var_weight[:, None, None] * (smooth(quantity_table - target) - pair_sums / (MEMBERS - 1))).astype(jnp.bfloat16)

    def backward(member_gradient):
        padded = cycle_pad(member_gradient)
        accumulated_outcome = jnp.zeros((C, NLAT * NLON), jnp.float32)
        for row_tap in range(3):
            for col_tap in range(3):
                window = padded[:, 2 - row_tap:2 - row_tap + NLAT, 2 - col_tap:2 - col_tap + NLON].reshape(OV, NLAT * NLON)
                accumulated_outcome = accumulated_outcome + jnp.dot(conv_weight[row_tap, col_tap].T, window, preferred_element_type=jnp.float32)
        return accumulated_outcome.reshape(C, NLAT, NLON).astype(jnp.bfloat16)
    input_slope_field = lax.map(backward, gradient)
    return (predicted_fields, input_slope_field)
```

```python
import functools

import jax
import jax.numpy as jnp
from jax import lax
from jax.experimental import pallas as pl
from jax.experimental.pallas import tpu as pltpu
from jax.sharding import PartitionSpec as P

MESH = pl.DeviceIdType.MESH
smoothing = 0.25
CHUNK = 16
f32, bf16 = jnp.float32, jnp.bfloat16


def smooth(difference):
    return difference * lax.rsqrt(difference * difference + smoothing * smoothing)


def kernel(
    sizes,
    x_ref, w_ref, obs_ref, bias_ref, var_ref,
    p_ref, out_ref,
    big, xt, wf, wbt, wb, pf, g, gs, others, latw,
    edge_out, edge_in, gedge_out, gedge_in,
    row_send, row_recv, grow_send, grow_recv,
    edge_send, edge_recv, gedge_send, gedge_recv, peer_send, peer_recv,
):
    members, lats, lons, channels, rows, cols, outputs, padded = sizes
    chunks = rows // CHUNK
    order = [0] + ([chunks - 1] if chunks > 1 else []) + list(range(1, chunks - 1))
    me, lat, lon = lax.axis_index("member"), lax.axis_index("lat"), lax.axis_index("lon")
    right, left = lax.rem(lon + 1, lons), lax.rem(lon + lons - 1, lons)
    has_up, has_down = lat > 0, lat < lats - 1

    barrier = pltpu.get_barrier_semaphore()
    for side in (left, right):
        pl.semaphore_signal(barrier, inc=1, device_id=(me, lat, side), device_id_type=MESH)

    @pl.when(has_up)
    def _():
        pl.semaphore_signal(barrier, inc=1, device_id=(me, lat - 1, lon), device_id_type=MESH)

    @pl.when(has_down)
    def _():
        pl.semaphore_signal(barrier, inc=1, device_id=(me, lat + 1, lon), device_id_type=MESH)

    def greet(step, carry):
        other = lax.rem(me + step, members)
        pl.semaphore_signal(barrier, inc=1, device_id=(other, lat, lon), device_id_type=MESH)
        return carry

    lax.fori_loop(1, members, greet, 0)

    def widen(c, carry):
        start = pl.multiple_of(c * rows, rows)
        big[pl.ds(start, rows), :] = x_ref[c].astype(f32)
        return carry

    lax.fori_loop(0, channels, widen, 0, unroll=4)

    def turn(r, carry):
        xt[r + 1] = big[pl.ds(r, channels, stride=rows), :].astype(bf16)
        return carry

    turn(0, 0)
    turn(rows - 1, 0)
    pl.semaphore_wait(barrier, members + 1 + has_up.astype(jnp.int32) + has_down.astype(jnp.int32))

    def row_copies(array, send, recv):
        up = pltpu.make_async_remote_copy(
            src_ref=array.at[1], dst_ref=array.at[rows + 1], send_sem=send.at[0],
            recv_sem=recv.at[0], device_id=(me, lat - 1, lon), device_id_type=MESH)
        down = pltpu.make_async_remote_copy(
            src_ref=array.at[rows], dst_ref=array.at[0], send_sem=send.at[1],
            recv_sem=recv.at[1], device_id=(me, lat + 1, lon), device_id_type=MESH)
        return up, down

    def start_up(copies):
        pl.when(has_up)(lambda: copies[0].start())

    def start_down(copies):
        pl.when(has_down)(lambda: copies[1].start())

    def wait_rows(copies, array):
        @pl.when(has_up)
        def _():
            copies[1].wait_recv()
            copies[0].wait_send()

        @pl.when(has_down)
        def _():
            copies[0].wait_recv()
            copies[1].wait_send()

        @pl.when(lat == 0)
        def _():
            array[0] = jnp.zeros(array.shape[1:], bf16)

        @pl.when(lat == lats - 1)
        def _():
            array[rows + 1] = jnp.zeros(array.shape[1:], bf16)

    x_rows = row_copies(xt, row_send, row_recv)
    start_up(x_rows)
    start_down(x_rows)
    lax.fori_loop(1, rows - 1, turn, 0)

    wf[...] = jnp.zeros(wf.shape, bf16)
    for a in range(3):
        for b in range(3):
            wf[b * padded : b * padded + outputs, a * channels : (a + 1) * channels] = w_ref[a, b]

    lane = lax.broadcasted_iota(jnp.int32, (padded, cols), 1)

    def forward(pair, q):
        rhs = jnp.concatenate(
            [xt[pl.ds(2 * pair + i, 3)].reshape(3 * channels, cols) for i in range(2)], axis=1)
        y = jnp.dot(wf[...], rhs, preferred_element_type=f32)
        for i in range(2):
            r = 2 * pair + i
            from_left, mid, from_right = [
                y[b * padded : (b + 1) * padded, i * cols : (i + 1) * cols] for b in range(3)]
            from_left = pltpu.roll(from_left, 1, 1)
            from_right = pltpu.roll(from_right, cols - 1, 1)
            edge_out[q, 0] = jnp.where(lane == r, pltpu.roll(from_left, r, 1), edge_out[q, 0])
            edge_out[q, 1] = jnp.where(lane == r, pltpu.roll(from_right, r + 1, 1), edge_out[q, 1])
            total = mid + jnp.where(lane == 0, 0.0, from_left)
            total = total + jnp.where(lane == cols - 1, 0.0, from_right)
            pf[pl.ds(r, padded, stride=rows), :] = total

    def edge_copies(q, source, target, send, recv):
        return [
            pltpu.make_async_remote_copy(
                src_ref=source.at[q, s], dst_ref=target.at[q, s], send_sem=send.at[q, s],
                recv_sem=recv.at[q, s], device_id=(me, lat, side), device_id_type=MESH)
            for s, side in enumerate((right, left))]

    def run_pairs(pairs, body):
        pairs = sorted(pairs)
        while pairs:
            n = 1
            while n < len(pairs) and pairs[n] == pairs[0] + n:
                n += 1

            def step(pair, carry):
                body(pair)
                return carry

            lax.fori_loop(pairs[0], pairs[0] + n, step, 0)
            pairs = pairs[n:]

    peer = lambda q, step: pltpu.make_async_remote_copy(
        src_ref=p_ref.at[:, pl.ds(q * CHUNK, CHUNK), :],
        dst_ref=others.at[step - 1, :, pl.ds(q * CHUNK, CHUNK), :],
        send_sem=peer_send.at[q, step - 1], recv_sem=peer_recv.at[q, step - 1],
        device_id=(lax.rem(me + step, members), lat, lon), device_id_type=MESH)

    edges = {}

    def finish(q):
        for copy in edges[q]:
            copy.wait()

        def fix(r, carry):
            at = pl.ds(r, padded, stride=rows)
            left_edge = pltpu.roll(edge_in[q, 0], lax.rem(cols - r, cols), 1)
            right_edge = pltpu.roll(edge_in[q, 1], cols - 1 - r, 1)
            total = pf[at, :]
            total = total + jnp.where(lane == 0, left_edge, 0.0)
            pf[at, :] = total + jnp.where(lane == cols - 1, right_edge, 0.0)
            return carry

        lax.fori_loop(q * CHUNK, (q + 1) * CHUNK, fix, 0)

        def pack(o, carry):
            at = pl.ds(pl.multiple_of(o * rows + q * CHUNK, CHUNK), CHUNK)
            p_ref[o, q * CHUNK : (q + 1) * CHUNK, :] = (pf[at, :] + bias_ref[o]).astype(bf16)
            return carry

        lax.fori_loop(0, outputs, pack, 0, unroll=3)

        def send(step, carry):
            peer(q, step).start()
            return carry

        lax.fori_loop(1, members, send, 0)

    half = CHUNK // 2
    waited = False
    for at, q in enumerate(order):
        edge_out[q] = jnp.zeros(edge_out.shape[1:], f32)
        pairs = range(q * half, (q + 1) * half)
        bounds = [p for p in pairs if p in (0, rows // 2 - 1)]
        run_pairs([p for p in pairs if p not in bounds], lambda p: forward(p, q))
        if bounds and not waited:
            wait_rows(x_rows, xt)
            waited = True
        for p in bounds:
            forward(p, q)
        edges[q] = edge_copies(q, edge_out, edge_in, edge_send, edge_recv)
        for copy in edges[q]:
            copy.start()
        if at:
            finish(order[at - 1])
    finish(order[-1])

    wbt[...] = jnp.zeros(wbt.shape, bf16)
    for a in range(3):
        for b in range(3):
            base = ((2 - a) * 3 + b) * padded
            wbt[base : base + outputs, :] = w_ref[a, b]
    wb[...] = jnp.transpose(wbt[...])
    row_index = (lat * rows + lax.broadcasted_iota(jnp.int32, (rows, cols), 0)).astype(f32)
    latw[...] = jnp.cos((-80.0 + 160.0 * (row_index + 0.5) / float(rows * lats)) * (jnp.pi / 180.0))

    def misfit(o, carry):
        at = pl.ds(pl.multiple_of(o * rows, rows), rows)
        g[at, :] = smooth(p_ref[o].astype(f32) - obs_ref[o].astype(f32))
        return carry

    lax.fori_loop(0, outputs, misfit, 0, unroll=3)
    g[pl.ds(outputs * rows, (padded - outputs) * rows), :] = jnp.zeros(
        ((padded - outputs) * rows, cols), f32)

    def gradient(q):
        inside = slice(q * CHUNK, (q + 1) * CHUNK)

        def arrive(step, carry):
            peer(q, step).wait()
            return carry

        lax.fori_loop(1, members, arrive, 0)
        weight_row = latw[inside, :]

        def score(o, carry):
            at = pl.ds(pl.multiple_of(o * rows + q * CHUNK, CHUNK), CHUNK)
            own = p_ref[o, inside, :].astype(f32)
            add = lambda j, run: run + smooth(own - others[j, o, inside, :].astype(f32))
            pair_sum = smooth(own - own)
            if members == 2:
                pair_sum = add(0, pair_sum)
            else:
                pair_sum = lax.fori_loop(0, members - 1, add, pair_sum)
            value = weight_row * var_ref[o] * (g[at, :] - pair_sum / (members - 1))
            g[at, :] = value.astype(bf16).astype(f32)
            return carry

        lax.fori_loop(0, outputs, score, 0, unroll=3)

        def collect(r, carry):
            to_right, to_left = carry
            row = g[pl.ds(r, padded, stride=rows), :]
            to_right = jnp.where(lane == r, pltpu.roll(row, r + 1, 1), to_right)
            to_left = jnp.where(lane == r, pltpu.roll(row, r, 1), to_left)
            return to_right, to_left

        zero = jnp.zeros((padded, cols), f32)
        gedge_out[q, 0], gedge_out[q, 1] = lax.fori_loop(
            q * CHUNK, (q + 1) * CHUNK, collect, (zero, zero))
        copies = edge_copies(q, gedge_out, gedge_in, gedge_send, gedge_recv)
        for copy in copies:
            copy.start()
        return copies

    def shifted(q):
        def one(r, carry):
            row = g[pl.ds(r, padded, stride=rows), :]
            left_edge = pltpu.roll(gedge_in[q, 0], lax.rem(cols - r, cols), 1)
            right_edge = pltpu.roll(gedge_in[q, 1], cols - 1 - r, 1)
            ahead = jnp.where(lane == cols - 1, right_edge, pltpu.roll(row, cols - 1, 1))
            behind = jnp.where(lane == 0, left_edge, pltpu.roll(row, 1, 1))
            gs[r + 1, 0:padded, :] = ahead.astype(bf16)
            gs[r + 1, padded : 2 * padded, :] = row.astype(bf16)
            gs[r + 1, 2 * padded :, :] = behind.astype(bf16)
            return carry

        lax.fori_loop(q * CHUNK, (q + 1) * CHUNK, one, 0)

    def backward(pair):
        rhs = jnp.concatenate(
            [gs[pl.ds(2 * pair + i, 3)].reshape(9 * padded, cols) for i in range(2)], axis=1)
        y = jnp.dot(wb[:, : 9 * padded], rhs, preferred_element_type=f32)
        for i in range(2):
            big[pl.ds(2 * pair + i, channels, stride=rows), :] = y[:, i * cols : (i + 1) * cols]

    g_rows = row_copies(gs, grow_send, grow_recv)
    ready, done = set(), set()

    def runnable():
        new = [p for p in range(1, rows // 2 - 1)
               if p not in done and {2 * p - 1, 2 * p, 2 * p + 1, 2 * p + 2} <= ready]
        done.update(new)
        return new

    for at, q in enumerate(order):
        copies = gradient(q)
        if at == len(order) - 1:
            if len(order) > 2:
                wait_rows(g_rows, gs)
                run_pairs([0], backward)
                run_pairs([rows // 2 - 1], backward)
        for copy in copies:
            copy.wait()
        shifted(q)
        ready.update(range(q * CHUNK, (q + 1) * CHUNK))
        if q == 0:
            start_up(g_rows)
        if q == chunks - 1:
            start_down(g_rows)
        run_pairs(runnable(), backward)
    if len(order) <= 2:
        wait_rows(g_rows, gs)
        run_pairs([0], backward)
        run_pairs([rows // 2 - 1], backward)

    def narrow(c, carry):
        start = pl.multiple_of(c * rows, rows)
        out_ref[c] = big[pl.ds(start, rows), :].astype(bf16)
        return carry

    lax.fori_loop(0, channels, narrow, 0, unroll=4)


def shards(layer_inputs, conv_weight, channel_offset, observed, var_weight):
    _, channels, rows, cols = layer_inputs.shape
    outputs = conv_weight.shape[2]
    members, lats, lons = [lax.axis_size(n) for n in ("member", "lat", "lon")]
    padded = -(-outputs // 16) * 16
    chunks = rows // CHUNK
    sizes = (members, lats, lons, channels, rows, cols, outputs, padded)
    vmem = pl.BlockSpec(memory_space=pltpu.VMEM)
    smem = pl.BlockSpec(memory_space=pltpu.SMEM)
    edge = pltpu.VMEM((chunks, 2, padded, cols), f32)
    dma = pltpu.SemaphoreType.DMA
    predicted, slope = pl.pallas_call(
        functools.partial(kernel, sizes),
        out_shape=(
            jax.ShapeDtypeStruct((outputs, rows, cols), bf16),
            jax.ShapeDtypeStruct((channels, rows, cols), bf16),
        ),
        in_specs=[vmem, vmem, vmem, smem, smem],
        out_specs=(vmem, vmem),
        scratch_shapes=[
            pltpu.VMEM((channels * rows, cols), f32),
            pltpu.VMEM((rows + 2, channels, cols), bf16),
            pltpu.VMEM((3 * padded, 3 * channels), bf16),
            pltpu.VMEM((-(-9 * padded // 128) * 128, channels), bf16),
            pltpu.VMEM((channels, -(-9 * padded // 128) * 128), bf16),
            pltpu.VMEM((padded * rows, cols), f32),
            pltpu.VMEM((padded * rows, cols), f32),
            pltpu.VMEM((rows + 2, 3 * padded, cols), bf16),
            pltpu.VMEM((members - 1, outputs, rows, cols), bf16),
            pltpu.VMEM((rows, cols), f32),
            edge, edge, edge, edge,
            dma((2,)), dma((2,)), dma((2,)), dma((2,)),
            dma((chunks, 2)), dma((chunks, 2)), dma((chunks, 2)), dma((chunks, 2)),
            dma((chunks, members - 1)), dma((chunks, members - 1)),
        ],
        compiler_params=pltpu.CompilerParams(
            collective_id=0, has_side_effects=True, vmem_limit_bytes=60 * 1024 * 1024),
        name="crps_step",
    )(layer_inputs[0], conv_weight, observed, channel_offset, var_weight)
    return predicted[None], slope[None]


def solution(mesh):
    in_specs = (P("member", None, "lat", "lon"), P(), P(), P(None, "lat", "lon"), P())
    out_specs = (P("member", None, "lat", "lon"), P("member", None, "lat", "lon"))
    return jax.shard_map(shards, mesh=mesh, in_specs=in_specs, out_specs=out_specs, check_vma=False)
```

```python
import functools

import jax
import jax.numpy as jnp
from jax import lax
from jax.experimental import pallas as pl
from jax.experimental.pallas import tpu as pltpu
from jax.sharding import PartitionSpec as P

MESH = pl.DeviceIdType.MESH
smoothing = 0.25
CHUNK = 16
f32, bf16 = jnp.float32, jnp.bfloat16


def smooth(difference):
    return difference * lax.rsqrt(difference * difference + smoothing * smoothing)


def pitch_of(rows):
    return rows + 8 if rows // 8 % 2 == 0 else rows


def kernel(
    sizes,
    x_ref, w_ref, obs_ref, bias_ref, var_ref,
    p_ref, out_ref,
    big, xt, wf, wbt, wb, pf, g, gs, others, latw,
    edge_out, edge_in, gedge_out, gedge_in,
    row_send, row_recv, grow_send, grow_recv,
    edge_send, edge_recv, gedge_send, gedge_recv, peer_send, peer_recv,
):
    members, lats, lons, channels, rows, cols, outputs, padded = sizes
    pitch = pitch_of(rows)
    chunks = rows // CHUNK
    order = [0] + ([chunks - 1] if chunks > 1 else []) + list(range(1, chunks - 1))
    me, lat, lon = lax.axis_index("member"), lax.axis_index("lat"), lax.axis_index("lon")
    right, left = lax.rem(lon + 1, lons), lax.rem(lon + lons - 1, lons)
    has_up, has_down = lat > 0, lat < lats - 1

    barrier = pltpu.get_barrier_semaphore()
    for side in (left, right):
        pl.semaphore_signal(barrier, inc=1, device_id=(me, lat, side), device_id_type=MESH)

    @pl.when(has_up)
    def _():
        pl.semaphore_signal(barrier, inc=1, device_id=(me, lat - 1, lon), device_id_type=MESH)

    @pl.when(has_down)
    def _():
        pl.semaphore_signal(barrier, inc=1, device_id=(me, lat + 1, lon), device_id_type=MESH)

    def greet(step, carry):
        other = lax.rem(me + step, members)
        pl.semaphore_signal(barrier, inc=1, device_id=(other, lat, lon), device_id_type=MESH)
        return carry

    lax.fori_loop(1, members, greet, 0)

    def widen(c, carry):
        start = pl.multiple_of(c * pitch, 8)
        big[pl.ds(start, rows), :] = x_ref[c].astype(f32)
        return carry

    lax.fori_loop(0, channels, widen, 0, unroll=4)

    def turn(r, carry):
        xt[r + 1] = big[pl.ds(r, channels, stride=pitch), :].astype(bf16)
        return carry

    turn(0, 0)
    turn(rows - 1, 0)
    pl.semaphore_wait(barrier, members + 1 + has_up.astype(jnp.int32) + has_down.astype(jnp.int32))

    def row_copies(array, send, recv):
        up = pltpu.make_async_remote_copy(
            src_ref=array.at[1], dst_ref=array.at[rows + 1], send_sem=send.at[0],
            recv_sem=recv.at[0], device_id=(me, lat - 1, lon), device_id_type=MESH)
        down = pltpu.make_async_remote_copy(
            src_ref=array.at[rows], dst_ref=array.at[0], send_sem=send.at[1],
            recv_sem=recv.at[1], device_id=(me, lat + 1, lon), device_id_type=MESH)
        return up, down

    def start_up(copies):
        pl.when(has_up)(lambda: copies[0].start())

    def start_down(copies):
        pl.when(has_down)(lambda: copies[1].start())

    def wait_rows(copies, array):
        @pl.when(has_up)
        def _():
            copies[1].wait_recv()
            copies[0].wait_send()

        @pl.when(has_down)
        def _():
            copies[0].wait_recv()
            copies[1].wait_send()

        @pl.when(lat == 0)
        def _():
            array[0] = jnp.zeros(array.shape[1:], bf16)

        @pl.when(lat == lats - 1)
        def _():
            array[rows + 1] = jnp.zeros(array.shape[1:], bf16)

    x_rows = row_copies(xt, row_send, row_recv)
    start_up(x_rows)
    start_down(x_rows)
    lax.fori_loop(1, rows - 1, turn, 0)

    wf[...] = jnp.zeros(wf.shape, bf16)
    for a in range(3):
        for b in range(3):
            wf[b * padded : b * padded + outputs, a * channels : (a + 1) * channels] = w_ref[a, b]

    lane = lax.broadcasted_iota(jnp.int32, (padded, cols), 1)

    def forward(pair, q):
        rhs = jnp.concatenate(
            [xt[pl.ds(2 * pair + i, 3)].reshape(3 * channels, cols) for i in range(2)], axis=1)
        y = jnp.dot(wf[...], rhs, preferred_element_type=f32)
        for i in range(2):
            r = 2 * pair + i
            from_left, mid, from_right = [
                y[b * padded : (b + 1) * padded, i * cols : (i + 1) * cols] for b in range(3)]
            from_left = pltpu.roll(from_left, 1, 1)
            from_right = pltpu.roll(from_right, cols - 1, 1)
            edge_out[q, 0] = jnp.where(lane == r, pltpu.roll(from_left, r, 1), edge_out[q, 0])
            edge_out[q, 1] = jnp.where(lane == r, pltpu.roll(from_right, r + 1, 1), edge_out[q, 1])
            total = mid + jnp.where(lane == 0, 0.0, from_left)
            total = total + jnp.where(lane == cols - 1, 0.0, from_right)
            pf[pl.ds(r, padded, stride=pitch), :] = total

    def edge_copies(q, source, target, send, recv):
        return [
            pltpu.make_async_remote_copy(
                src_ref=source.at[q, s], dst_ref=target.at[q, s], send_sem=send.at[q, s],
                recv_sem=recv.at[q, s], device_id=(me, lat, side), device_id_type=MESH)
            for s, side in enumerate((right, left))]

    def run_pairs(pairs, body):
        pairs = sorted(pairs)
        while pairs:
            n = 1
            while n < len(pairs) and pairs[n] == pairs[0] + n:
                n += 1

            def step(pair, carry):
                body(pair)
                return carry

            lax.fori_loop(pairs[0], pairs[0] + n, step, 0)
            pairs = pairs[n:]

    peer = lambda q, step: pltpu.make_async_remote_copy(
        src_ref=p_ref.at[:, pl.ds(q * CHUNK, CHUNK), :],
        dst_ref=others.at[step - 1, :, pl.ds(q * CHUNK, CHUNK), :],
        send_sem=peer_send.at[q, step - 1], recv_sem=peer_recv.at[q, step - 1],
        device_id=(lax.rem(me + step, members), lat, lon), device_id_type=MESH)

    edges = {}

    def finish(q):
        for copy in edges[q]:
            copy.wait()

        def fix(r, carry):
            at = pl.ds(r, padded, stride=pitch)
            left_edge = pltpu.roll(edge_in[q, 0], lax.rem(cols - r, cols), 1)
            right_edge = pltpu.roll(edge_in[q, 1], cols - 1 - r, 1)
            total = pf[at, :]
            total = total + jnp.where(lane == 0, left_edge, 0.0)
            pf[at, :] = total + jnp.where(lane == cols - 1, right_edge, 0.0)
            return carry

        lax.fori_loop(q * CHUNK, (q + 1) * CHUNK, fix, 0)

        def pack(o, carry):
            at = pl.ds(pl.multiple_of(o * pitch + q * CHUNK, 8), CHUNK)
            p_ref[o, q * CHUNK : (q + 1) * CHUNK, :] = (pf[at, :] + bias_ref[o]).astype(bf16)
            return carry

        lax.fori_loop(0, outputs, pack, 0, unroll=3)

        def send(step, carry):
            peer(q, step).start()
            return carry

        lax.fori_loop(1, members, send, 0)

    half = CHUNK // 2
    waited = False
    for at, q in enumerate(order):
        edge_out[q] = jnp.zeros(edge_out.shape[1:], f32)
        pairs = range(q * half, (q + 1) * half)
        bounds = [p for p in pairs if p in (0, rows // 2 - 1)]
        run_pairs([p for p in pairs if p not in bounds], lambda p: forward(p, q))
        if bounds and not waited:
            wait_rows(x_rows, xt)
            waited = True
        for p in bounds:
            forward(p, q)
        edges[q] = edge_copies(q, edge_out, edge_in, edge_send, edge_recv)
        for copy in edges[q]:
            copy.start()
        if at:
            finish(order[at - 1])
    wbt[...] = jnp.zeros(wbt.shape, bf16)
    for a in range(3):
        for b in range(3):
            base = ((2 - a) * 3 + b) * padded
            wbt[base : base + outputs, :] = w_ref[a, b]
    wb[...] = jnp.transpose(wbt[...])
    row_index = (lat * rows + lax.broadcasted_iota(jnp.int32, (rows, cols), 0)).astype(f32)
    latw[...] = jnp.cos((-80.0 + 160.0 * (row_index + 0.5) / float(rows * lats)) * (jnp.pi / 180.0))

    def misfits(q):
        inside = slice(q * CHUNK, (q + 1) * CHUNK)

        def misfit(o, carry):
            at = pl.ds(pl.multiple_of(o * pitch + q * CHUNK, 8), CHUNK)
            g[at, :] = smooth(p_ref[o, inside, :].astype(f32) - obs_ref[o, inside, :].astype(f32))
            return carry

        lax.fori_loop(0, outputs, misfit, 0, unroll=3)

    g[pl.ds(outputs * pitch, (padded - outputs) * pitch), :] = jnp.zeros(
        ((padded - outputs) * pitch, cols), f32)
    for q in order[:-1]:
        misfits(q)
    finish(order[-1])
    misfits(order[-1])

    def gradient(q):
        inside = slice(q * CHUNK, (q + 1) * CHUNK)

        def arrive(step, carry):
            peer(q, step).wait()
            return carry

        lax.fori_loop(1, members, arrive, 0)
        weight_row = latw[inside, :]

        def score(o, carry):
            at = pl.ds(pl.multiple_of(o * pitch + q * CHUNK, 8), CHUNK)
            own = p_ref[o, inside, :].astype(f32)
            add = lambda j, run: run + smooth(own - others[j, o, inside, :].astype(f32))
            pair_sum = smooth(own - own)
            if members == 2:
                pair_sum = add(0, pair_sum)
            else:
                pair_sum = lax.fori_loop(0, members - 1, add, pair_sum)
            value = weight_row * var_ref[o] * (g[at, :] - pair_sum / (members - 1))
            g[at, :] = value.astype(bf16).astype(f32)
            return carry

        lax.fori_loop(0, outputs, score, 0, unroll=3)

        def collect(r, carry):
            to_right, to_left = carry
            row = g[pl.ds(r, padded, stride=pitch), :]
            to_right = jnp.where(lane == r, pltpu.roll(row, r + 1, 1), to_right)
            to_left = jnp.where(lane == r, pltpu.roll(row, r, 1), to_left)
            return to_right, to_left

        zero = jnp.zeros((padded, cols), f32)
        gedge_out[q, 0], gedge_out[q, 1] = lax.fori_loop(
            q * CHUNK, (q + 1) * CHUNK, collect, (zero, zero))
        copies = edge_copies(q, gedge_out, gedge_in, gedge_send, gedge_recv)
        for copy in copies:
            copy.start()
        return copies

    def shifted(q):
        def one(r, carry):
            row = g[pl.ds(r, padded, stride=pitch), :]
            left_edge = pltpu.roll(gedge_in[q, 0], lax.rem(cols - r, cols), 1)
            right_edge = pltpu.roll(gedge_in[q, 1], cols - 1 - r, 1)
            ahead = jnp.where(lane == cols - 1, right_edge, pltpu.roll(row, cols - 1, 1))
            behind = jnp.where(lane == 0, left_edge, pltpu.roll(row, 1, 1))
            gs[r + 1, 0:padded, :] = ahead.astype(bf16)
            gs[r + 1, padded : 2 * padded, :] = row.astype(bf16)
            gs[r + 1, 2 * padded :, :] = behind.astype(bf16)
            return carry

        lax.fori_loop(q * CHUNK, (q + 1) * CHUNK, one, 0)

    def backward(pair):
        rhs = jnp.concatenate(
            [gs[pl.ds(2 * pair + i, 3)].reshape(9 * padded, cols) for i in range(2)], axis=1)
        y = jnp.dot(wb[:, : 9 * padded], rhs, preferred_element_type=f32)
        for i in range(2):
            big[pl.ds(2 * pair + i, channels, stride=pitch), :] = y[:, i * cols : (i + 1) * cols]

    g_rows = row_copies(gs, grow_send, grow_recv)
    ready, done = set(), set()

    def runnable():
        new = [p for p in range(1, rows // 2 - 1)
               if p not in done and {2 * p - 1, 2 * p, 2 * p + 1, 2 * p + 2} <= ready]
        done.update(new)
        return new

    def settle(q, copies):
        for copy in copies:
            copy.wait()
        shifted(q)
        ready.update(range(q * CHUNK, (q + 1) * CHUNK))
        if q == 0:
            start_up(g_rows)
        if q == chunks - 1:
            start_down(g_rows)

    early = order[:-1]
    moving = [(q, gradient(q)) for q in early]
    for q, copies in moving:
        settle(q, copies)
    work = runnable()
    run_pairs(work[: len(work) // 2], backward)
    last = order[-1]
    copies = gradient(last)
    run_pairs(work[len(work) // 2 :], backward)
    if len(order) > 2:
        wait_rows(g_rows, gs)
        run_pairs([0], backward)
        run_pairs([rows // 2 - 1], backward)
    settle(last, copies)
    run_pairs(runnable(), backward)
    if len(order) <= 2:
        wait_rows(g_rows, gs)
        run_pairs([0], backward)
        run_pairs([rows // 2 - 1], backward)

    def narrow(c, carry):
        start = pl.multiple_of(c * pitch, 8)
        out_ref[c] = big[pl.ds(start, rows), :].astype(bf16)
        return carry

    lax.fori_loop(0, channels, narrow, 0, unroll=4)


def shards(layer_inputs, conv_weight, channel_offset, observed, var_weight):
    _, channels, rows, cols = layer_inputs.shape
    outputs = conv_weight.shape[2]
    members, lats, lons = [lax.axis_size(n) for n in ("member", "lat", "lon")]
    padded = -(-outputs // 16) * 16
    chunks = rows // CHUNK
    sizes = (members, lats, lons, channels, rows, cols, outputs, padded)
    vmem = pl.BlockSpec(memory_space=pltpu.VMEM)
    smem = pl.BlockSpec(memory_space=pltpu.SMEM)
    edge = pltpu.VMEM((chunks, 2, padded, cols), f32)
    dma = pltpu.SemaphoreType.DMA
    predicted, slope = pl.pallas_call(
        functools.partial(kernel, sizes),
        out_shape=(
            pltpu.VMEM((outputs, rows, cols), bf16),
            pltpu.VMEM((channels, rows, cols), bf16),
        ),
        in_specs=[vmem, vmem, vmem, smem, smem],
        out_specs=(vmem, vmem),
        scratch_shapes=[
            pltpu.VMEM((channels * pitch_of(rows), cols), f32),
            pltpu.VMEM((rows + 2, channels, cols), bf16),
            pltpu.VMEM((3 * padded, 3 * channels), bf16),
            pltpu.VMEM((-(-9 * padded // 128) * 128, channels), bf16),
            pltpu.VMEM((channels, -(-9 * padded // 128) * 128), bf16),
            pltpu.VMEM((padded * pitch_of(rows), cols), f32),
            pltpu.VMEM((padded * pitch_of(rows), cols), f32),
            pltpu.VMEM((rows + 2, 3 * padded, cols), bf16),
            pltpu.VMEM((members - 1, outputs, rows, cols), bf16),
            pltpu.VMEM((rows, cols), f32),
            edge, edge, edge, edge,
            dma((2,)), dma((2,)), dma((2,)), dma((2,)),
            dma((chunks, 2)), dma((chunks, 2)), dma((chunks, 2)), dma((chunks, 2)),
            dma((chunks, members - 1)), dma((chunks, members - 1)),
        ],
        compiler_params=pltpu.CompilerParams(
            collective_id=0, has_side_effects=True, vmem_limit_bytes=60 * 1024 * 1024),
        name="crps_step",
    )(layer_inputs[0], conv_weight, observed, channel_offset, var_weight)
    return predicted[None], slope[None]


def solution(mesh):
    in_specs = (P("member", None, "lat", "lon"), P(), P(), P(None, "lat", "lon"), P())
    out_specs = (P("member", None, "lat", "lon"), P("member", None, "lat", "lon"))
    return jax.shard_map(shards, mesh=mesh, in_specs=in_specs, out_specs=out_specs, check_vma=False)
```

```python
import functools
import math

import jax
import jax.numpy as jnp
from jax import lax
from jax.experimental import pallas as pl
from jax.experimental.pallas import tpu as pltpu
from jax.sharding import PartitionSpec as P

MESH = pl.DeviceIdType.MESH
smoothing = 0.25
CHUNK = 16
f32, bf16 = jnp.float32, jnp.bfloat16


def smooth(difference):
    return difference * lax.rsqrt(difference * difference + smoothing * smoothing)


def pitch_of(rows):
    return rows + 8 if rows // 8 % 2 == 0 else rows


def kernel(
    sizes,
    x_hbm, w_hbm, obs_hbm, bias_ref, var_ref,
    p_ref, out_ref,
    x_ref, w_ref, obs_ref, load_sem, big, xt, wf, wbt, wb, pf, g, gs, others, latw,
    turned, edge_out, edge_in, gedge_out, gedge_in,
    row_send, row_recv, grow_send, grow_recv,
    edge_send, edge_recv, gedge_send, gedge_recv, peer_send, peer_recv,
):
    members, lats, lons, channels, rows, cols, outputs, padded = sizes
    pitch = pitch_of(rows)
    spread = max(d for d in range(1, 25) if outputs % d == 0)
    chunks = rows // CHUNK
    order = [0] + ([chunks - 1] if chunks > 1 else []) + list(range(1, chunks - 1))
    me, lat, lon = lax.axis_index("member"), lax.axis_index("lat"), lax.axis_index("lon")
    right, left = lax.rem(lon + 1, lons), lax.rem(lon + lons - 1, lons)
    has_up, has_down = lat > 0, lat < lats - 1

    loads = {
        q: pltpu.make_async_copy(
            x_hbm.at[:, pl.ds(q * CHUNK, CHUNK), :], x_ref.at[:, pl.ds(q * CHUNK, CHUNK), :],
            load_sem.at[q])
        for q in order}
    loads["w"] = pltpu.make_async_copy(w_hbm, w_ref, load_sem.at[chunks])
    loads["obs"] = pltpu.make_async_copy(obs_hbm, obs_ref, load_sem.at[chunks + 1])
    for load in loads.values():
        load.start()

    barrier = pltpu.get_barrier_semaphore()
    for side in (left, right):
        pl.semaphore_signal(barrier, inc=1, device_id=(me, lat, side), device_id_type=MESH)

    @pl.when(has_up)
    def _():
        pl.semaphore_signal(barrier, inc=1, device_id=(me, lat - 1, lon), device_id_type=MESH)

    @pl.when(has_down)
    def _():
        pl.semaphore_signal(barrier, inc=1, device_id=(me, lat + 1, lon), device_id_type=MESH)

    def greet(step, carry):
        other = lax.rem(me + step, members)
        pl.semaphore_signal(barrier, inc=1, device_id=(other, lat, lon), device_id_type=MESH)
        return carry

    lax.fori_loop(1, members, greet, 0)

    def widen(q):
        loads[q].wait()

        def one(c, carry):
            at = pl.ds(pl.multiple_of(c * pitch + q * CHUNK, 8), CHUNK)
            big[at, :] = x_ref[c, q * CHUNK : (q + 1) * CHUNK, :].astype(f32)
            return carry

        lax.fori_loop(0, channels, one, 0, unroll=16)

    def turn(r, carry):
        xt[r + 1] = big[pl.ds(r, channels, stride=pitch), :].astype(bf16)
        return carry

    for q in order[:2]:
        widen(q)
    turn(0, 0)
    turn(rows - 1, 0)
    pl.semaphore_wait(barrier, members + 1 + has_up.astype(jnp.int32) + has_down.astype(jnp.int32))

    def row_copies(array, send, recv):
        up = pltpu.make_async_remote_copy(
            src_ref=array.at[1], dst_ref=array.at[rows + 1], send_sem=send.at[0],
            recv_sem=recv.at[0], device_id=(me, lat - 1, lon), device_id_type=MESH)
        down = pltpu.make_async_remote_copy(
            src_ref=array.at[rows], dst_ref=array.at[0], send_sem=send.at[1],
            recv_sem=recv.at[1], device_id=(me, lat + 1, lon), device_id_type=MESH)
        return up, down

    def start_up(copies):
        pl.when(has_up)(lambda: copies[0].start())

    def start_down(copies):
        pl.when(has_down)(lambda: copies[1].start())

    def wait_rows(copies, array):
        @pl.when(has_up)
        def _():
            copies[1].wait_recv()
            copies[0].wait_send()

        @pl.when(has_down)
        def _():
            copies[0].wait_recv()
            copies[1].wait_send()

        @pl.when(lat == 0)
        def _():
            array[0] = jnp.zeros(array.shape[1:], bf16)

        @pl.when(lat == lats - 1)
        def _():
            array[rows + 1] = jnp.zeros(array.shape[1:], bf16)

    x_rows = row_copies(xt, row_send, row_recv)
    start_up(x_rows)
    start_down(x_rows)
    lax.fori_loop(1, CHUNK, turn, 0, unroll=3)
    if chunks > 1:
        lax.fori_loop(rows - CHUNK, rows - 1, turn, 0, unroll=3)
    for q in order[2:]:
        widen(q)
        lax.fori_loop(q * CHUNK, (q + 1) * CHUNK, turn, 0, unroll=2)
    loads["w"].wait()

    wf[...] = jnp.zeros(wf.shape, bf16)
    for a in range(3):
        for b in range(3):
            wf[b * padded : b * padded + outputs, a * channels : (a + 1) * channels] = w_ref[a, b]

    lane = lax.broadcasted_iota(jnp.int32, (padded, cols), 1)
    thin = lax.broadcasted_iota(jnp.int32, (CHUNK, cols), 1)

    def forward(pair, q):
        rhs = jnp.concatenate(
            [xt[pl.ds(2 * pair + i, 3)].reshape(3 * channels, cols) for i in range(2)], axis=1)
        y = jnp.dot(wf[...], rhs, preferred_element_type=f32)
        for i in range(2):
            r = 2 * pair + i
            from_left, mid, from_right = [
                y[b * padded : (b + 1) * padded, i * cols : (i + 1) * cols] for b in range(3)]
            from_left = pltpu.roll(from_left, 1, 1)
            from_right = pltpu.roll(from_right, cols - 1, 1)
            slot = r - q * CHUNK
            both = pltpu.roll(jnp.where(lane == 0, from_left, from_right), 2 * slot + 1, 1)
            turned[0, 0:padded, :] = jnp.where(lane // 2 == slot, both, turned[0, 0:padded, :])
            total = mid + jnp.where(lane == 0, 0.0, from_left)
            total = total + jnp.where(lane == cols - 1, 0.0, from_right)
            pf[pl.ds(r, padded, stride=pitch), :] = total

    def edge_copies(q, source, target, send, recv):
        return [
            pltpu.make_async_remote_copy(
                src_ref=source.at[q, s], dst_ref=target.at[q, s], send_sem=send.at[q, s],
                recv_sem=recv.at[q, s], device_id=(me, lat, side), device_id_type=MESH)
            for s, side in enumerate((right, left))]

    def run_pairs(pairs, body):
        pairs = sorted(pairs)
        while pairs:
            n = 1
            while n < len(pairs) and pairs[n] == pairs[0] + n:
                n += 1

            def step(pair, carry):
                body(pair)
                return carry

            lax.fori_loop(pairs[0], pairs[0] + n, step, 0, unroll=math.gcd(n, 2) if n % 2 == 0 else n if n < 8 else 1)
            pairs = pairs[n:]

    peer = lambda q, step: pltpu.make_async_remote_copy(
        src_ref=p_ref.at[:, pl.ds(q * CHUNK, CHUNK), :],
        dst_ref=others.at[step - 1, :, pl.ds(q * CHUNK, CHUNK), :],
        send_sem=peer_send.at[q, step - 1], recv_sem=peer_recv.at[q, step - 1],
        device_id=(lax.rem(me + step, members), lat, lon), device_id_type=MESH)

    edges = {}

    def finish(q):
        for copy in edges[q]:
            copy.wait()

        left_edge, right_edge = edge_in[q, 0], edge_in[q, 1]

        def pack(o, carry):
            at = pl.ds(pl.multiple_of(o * pitch + q * CHUNK, 8), CHUNK)
            total = pf[at, :]
            total = total + jnp.where(thin == 0, pltpu.roll(left_edge, lax.rem(cols - o, cols), 1), 0.0)
            total = total + jnp.where(thin == cols - 1, pltpu.roll(right_edge, cols - 1 - o, 1), 0.0)
            p_ref[o, q * CHUNK : (q + 1) * CHUNK, :] = (total + bias_ref[o]).astype(bf16)
            return carry

        lax.fori_loop(0, outputs, pack, 0, unroll=spread)

        def send(step, carry):
            peer(q, step).start()
            return carry

        lax.fori_loop(1, members, send, 0)

    half = CHUNK // 2
    turned[0] = jnp.zeros(turned.shape[1:], f32)
    waited = False
    for at, q in enumerate(order):
        pairs = range(q * half, (q + 1) * half)
        bounds = [p for p in pairs if p in (0, rows // 2 - 1)]
        run_pairs([p for p in pairs if p not in bounds], lambda p: forward(p, q))
        if bounds and not waited:
            wait_rows(x_rows, xt)
            waited = True
        for p in bounds:
            forward(p, q)
        turned[1] = jnp.transpose(turned[0])
        edge_out[q, 0] = turned[1, pl.ds(1, CHUNK, stride=2), :]
        edge_out[q, 1] = turned[1, pl.ds(0, CHUNK, stride=2), :]
        edges[q] = edge_copies(q, edge_out, edge_in, edge_send, edge_recv)
        for copy in edges[q]:
            copy.start()
        if at:
            finish(order[at - 1])
    wbt[...] = jnp.zeros(wbt.shape, bf16)
    for a in range(3):
        for b in range(3):
            base = ((2 - a) * 3 + b) * padded
            wbt[base : base + outputs, :] = w_ref[a, b]
    wb[...] = jnp.transpose(wbt[...])
    row_index = (lat * rows + lax.broadcasted_iota(jnp.int32, (rows, cols), 0)).astype(f32)
    latw[...] = jnp.cos((-80.0 + 160.0 * (row_index + 0.5) / float(rows * lats)) * (jnp.pi / 180.0))

    loads["obs"].wait()

    def misfits(q):
        inside = slice(q * CHUNK, (q + 1) * CHUNK)

        def misfit(o, carry):
            at = pl.ds(pl.multiple_of(o * pitch + q * CHUNK, 8), CHUNK)
            g[at, :] = smooth(p_ref[o, inside, :].astype(f32) - obs_ref[o, inside, :].astype(f32))
            return carry

        lax.fori_loop(0, outputs, misfit, 0, unroll=spread)

    g[pl.ds(outputs * pitch, (padded - outputs) * pitch), :] = jnp.zeros(
        ((padded - outputs) * pitch, cols), f32)
    for q in order[:-1]:
        misfits(q)
    finish(order[-1])
    misfits(order[-1])

    def gradient(q):
        inside = slice(q * CHUNK, (q + 1) * CHUNK)

        def arrive(step, carry):
            peer(q, step).wait()
            return carry

        lax.fori_loop(1, members, arrive, 0)
        weight_row = latw[inside, :]

        def score(o, carry):
            at = pl.ds(pl.multiple_of(o * pitch + q * CHUNK, 8), CHUNK)
            own = p_ref[o, inside, :].astype(f32)
            add = lambda j, run: run + smooth(own - others[j, o, inside, :].astype(f32))
            pair_sum = smooth(own - own)
            if members == 2:
                pair_sum = add(0, pair_sum)
            else:
                pair_sum = lax.fori_loop(0, members - 1, add, pair_sum)
            value = weight_row * var_ref[o] * (g[at, :] - pair_sum / (members - 1))
            value = value.astype(bf16).astype(f32)
            g[at, :] = value
            to_right, to_left = carry
            to_right = jnp.where(thin == o, pltpu.roll(value, o + 1, 1), to_right)
            to_left = jnp.where(thin == o, pltpu.roll(value, o, 1), to_left)
            return to_right, to_left

        zero = jnp.zeros((CHUNK, cols), f32)
        gedge_out[q, 0], gedge_out[q, 1] = lax.fori_loop(
            0, outputs, score, (zero, zero), unroll=spread)
        copies = edge_copies(q, gedge_out, gedge_in, gedge_send, gedge_recv)
        for copy in copies:
            copy.start()
        return copies

    def shifted(q):
        turned[1, pl.ds(0, CHUNK, stride=2), :] = gedge_in[q, 1]
        turned[1, pl.ds(1, CHUNK, stride=2), :] = gedge_in[q, 0]
        turned[0] = jnp.transpose(turned[1])

        def one(r, carry):
            row = g[pl.ds(r, padded, stride=pitch), :]
            both = pltpu.roll(turned[0, 0:padded, :], cols - 1 - 2 * (r - q * CHUNK), 1)
            ahead = jnp.where(lane == cols - 1, both, pltpu.roll(row, cols - 1, 1))
            behind = jnp.where(lane == 0, both, pltpu.roll(row, 1, 1))
            gs[r + 1, 0:padded, :] = ahead.astype(bf16)
            gs[r + 1, padded : 2 * padded, :] = row.astype(bf16)
            gs[r + 1, 2 * padded :, :] = behind.astype(bf16)
            return carry

        lax.fori_loop(q * CHUNK, (q + 1) * CHUNK, one, 0, unroll=4)

    def backward(pair):
        rhs = jnp.concatenate(
            [gs[pl.ds(2 * pair + i, 3)].reshape(9 * padded, cols) for i in range(2)], axis=1)
        y = jnp.dot(wb[:, : 9 * padded], rhs, preferred_element_type=f32)
        for i in range(2):
            big[pl.ds(2 * pair + i, channels, stride=pitch), :] = y[:, i * cols : (i + 1) * cols]

    g_rows = row_copies(gs, grow_send, grow_recv)
    ready, done = set(), set()

    def runnable():
        new = [p for p in range(1, rows // 2 - 1)
               if p not in done and {2 * p - 1, 2 * p, 2 * p + 1, 2 * p + 2} <= ready]
        done.update(new)
        return new

    def settle(q, copies):
        for copy in copies:
            copy.wait()
        shifted(q)
        ready.update(range(q * CHUNK, (q + 1) * CHUNK))
        if q == 0:
            start_up(g_rows)
        if q == chunks - 1:
            start_down(g_rows)

    early = order[:-1]
    moving = [(q, gradient(q)) for q in early]
    for q, copies in moving:
        settle(q, copies)
    work = runnable()
    run_pairs(work[: len(work) // 2], backward)
    last = order[-1]
    copies = gradient(last)
    run_pairs(work[len(work) // 2 :], backward)
    if len(order) > 2:
        wait_rows(g_rows, gs)
        run_pairs([0], backward)
        run_pairs([rows // 2 - 1], backward)
    settle(last, copies)
    run_pairs(runnable(), backward)
    if len(order) <= 2:
        wait_rows(g_rows, gs)
        run_pairs([0], backward)
        run_pairs([rows // 2 - 1], backward)

    def narrow(c, carry):
        start = pl.multiple_of(c * pitch, 8)
        out_ref[c] = big[pl.ds(start, rows), :].astype(bf16)
        return carry

    lax.fori_loop(0, channels, narrow, 0, unroll=8)


def shards(layer_inputs, conv_weight, channel_offset, observed, var_weight):
    _, channels, rows, cols = layer_inputs.shape
    outputs = conv_weight.shape[2]
    members, lats, lons = [lax.axis_size(n) for n in ("member", "lat", "lon")]
    padded = -(-outputs // 16) * 16
    chunks = rows // CHUNK
    sizes = (members, lats, lons, channels, rows, cols, outputs, padded)
    vmem = pl.BlockSpec(memory_space=pltpu.VMEM)
    smem = pl.BlockSpec(memory_space=pltpu.SMEM)
    edge = pltpu.VMEM((chunks, 2, CHUNK, cols), f32)
    hbm = pl.BlockSpec(memory_space=pl.ANY)
    dma = pltpu.SemaphoreType.DMA
    predicted, slope = pl.pallas_call(
        functools.partial(kernel, sizes),
        out_shape=(
            pltpu.VMEM((outputs, rows, cols), bf16),
            pltpu.VMEM((channels, rows, cols), bf16),
        ),
        in_specs=[hbm, hbm, hbm, smem, smem],
        out_specs=(vmem, vmem),
        scratch_shapes=[
            pltpu.VMEM((channels, rows, cols), bf16),
            pltpu.VMEM(conv_weight.shape, bf16),
            pltpu.VMEM((outputs, rows, cols), bf16),
            dma((chunks + 2,)),
            pltpu.VMEM((channels * pitch_of(rows), cols), f32),
            pltpu.VMEM((rows + 2, channels, cols), bf16),
            pltpu.VMEM((3 * padded, 3 * channels), bf16),
            pltpu.VMEM((-(-9 * padded // 128) * 128, channels), bf16),
            pltpu.VMEM((channels, -(-9 * padded // 128) * 128), bf16),
            pltpu.VMEM((padded * pitch_of(rows), cols), f32),
            pltpu.VMEM((padded * pitch_of(rows), cols), f32),
            pltpu.VMEM((rows + 2, 3 * padded, cols), bf16),
            pltpu.VMEM((members - 1, outputs, rows, cols), bf16),
            pltpu.VMEM((rows, cols), f32),
            pltpu.VMEM((2, cols, cols), f32),
            edge, edge, edge, edge,
            dma((2,)), dma((2,)), dma((2,)), dma((2,)),
            dma((chunks, 2)), dma((chunks, 2)), dma((chunks, 2)), dma((chunks, 2)),
            dma((chunks, members - 1)), dma((chunks, members - 1)),
        ],
        compiler_params=pltpu.CompilerParams(
            collective_id=0, has_side_effects=True, vmem_limit_bytes=60 * 1024 * 1024),
        name="crps_step",
    )(layer_inputs[0], conv_weight, observed, channel_offset, var_weight)
    return predicted[None], slope[None]


def solution(mesh):
    in_specs = (P("member", None, "lat", "lon"), P(), P(), P(None, "lat", "lon"), P())
    out_specs = (P("member", None, "lat", "lon"), P("member", None, "lat", "lon"))
    return jax.shard_map(shards, mesh=mesh, in_specs=in_specs, out_specs=out_specs, check_vma=False)
```

```python
import functools
import math

import jax
import jax.numpy as jnp
from jax import lax
from jax.experimental import pallas as pl
from jax.experimental.pallas import tpu as pltpu
from jax.sharding import PartitionSpec as P

MESH = pl.DeviceIdType.MESH
smoothing = 0.25
CHUNK = 16
f32, bf16 = jnp.float32, jnp.bfloat16


def smooth(difference):
    return difference * lax.rsqrt(difference * difference + smoothing * smoothing)


def pitch_of(rows):
    return rows + 8 if rows // 8 % 2 == 0 else rows


def kernel(
    sizes,
    x_hbm, w_hbm, obs_hbm, bias_ref, var_ref,
    p_ref, out_ref,
    x_ref, w_ref, obs_ref, load_sem, big, xt, wf, wbt, wb, pf, g, gs, others, latw,
    turned, edge_out, edge_in, gedge_out, gedge_in,
    row_send, row_recv, grow_send, grow_recv,
    edge_send, edge_recv, gedge_send, gedge_recv, peer_send, peer_recv,
):
    members, lats, lons, channels, rows, cols, outputs, padded = sizes
    pitch = pitch_of(rows)
    spread = max(d for d in range(1, 25) if outputs % d == 0)
    chunks = rows // CHUNK
    order = [0] + ([chunks - 1] if chunks > 1 else []) + list(range(1, chunks - 1))
    me, lat, lon = lax.axis_index("member"), lax.axis_index("lat"), lax.axis_index("lon")
    right, left = lax.rem(lon + 1, lons), lax.rem(lon + lons - 1, lons)
    has_up, has_down = lat > 0, lat < lats - 1

    loads = {
        q: pltpu.make_async_copy(
            x_hbm.at[:, pl.ds(q * CHUNK, CHUNK), :], x_ref.at[:, pl.ds(q * CHUNK, CHUNK), :],
            load_sem.at[q])
        for q in order}
    loads["w"] = pltpu.make_async_copy(w_hbm, w_ref, load_sem.at[chunks])
    loads["obs"] = pltpu.make_async_copy(obs_hbm, obs_ref, load_sem.at[chunks + 1])
    for load in loads.values():
        load.start()

    barrier = pltpu.get_barrier_semaphore()
    for side in (left, right):
        pl.semaphore_signal(barrier, inc=1, device_id=(me, lat, side), device_id_type=MESH)

    @pl.when(has_up)
    def _():
        pl.semaphore_signal(barrier, inc=1, device_id=(me, lat - 1, lon), device_id_type=MESH)

    @pl.when(has_down)
    def _():
        pl.semaphore_signal(barrier, inc=1, device_id=(me, lat + 1, lon), device_id_type=MESH)

    def greet(step, carry):
        other = lax.rem(me + step, members)
        pl.semaphore_signal(barrier, inc=1, device_id=(other, lat, lon), device_id_type=MESH)
        return carry

    lax.fori_loop(1, members, greet, 0)

    def widen(q):
        loads[q].wait()

        def one(c, carry):
            at = pl.ds(pl.multiple_of(c * pitch + q * CHUNK, 8), CHUNK)
            big[at, :] = x_ref[c, q * CHUNK : (q + 1) * CHUNK, :].astype(f32)
            return carry

        lax.fori_loop(0, channels, one, 0, unroll=16)

    def turn(r, carry):
        xt[r + 1] = big[pl.ds(r, channels, stride=pitch), :].astype(bf16)
        return carry

    for q in order[:2]:
        widen(q)
    turn(0, 0)
    turn(rows - 1, 0)
    pl.semaphore_wait(barrier, members + 1 + has_up.astype(jnp.int32) + has_down.astype(jnp.int32))

    def row_copies(array, send, recv):
        up = pltpu.make_async_remote_copy(
            src_ref=array.at[1], dst_ref=array.at[rows + 1], send_sem=send.at[0],
            recv_sem=recv.at[0], device_id=(me, lat - 1, lon), device_id_type=MESH)
        down = pltpu.make_async_remote_copy(
            src_ref=array.at[rows], dst_ref=array.at[0], send_sem=send.at[1],
            recv_sem=recv.at[1], device_id=(me, lat + 1, lon), device_id_type=MESH)
        return up, down

    def start_up(copies):
        pl.when(has_up)(lambda: copies[0].start())

    def start_down(copies):
        pl.when(has_down)(lambda: copies[1].start())

    def wait_rows(copies, array):
        @pl.when(has_up)
        def _():
            copies[1].wait_recv()
            copies[0].wait_send()

        @pl.when(has_down)
        def _():
            copies[0].wait_recv()
            copies[1].wait_send()

        @pl.when(lat == 0)
        def _():
            array[0] = jnp.zeros(array.shape[1:], bf16)

        @pl.when(lat == lats - 1)
        def _():
            array[rows + 1] = jnp.zeros(array.shape[1:], bf16)

    x_rows = row_copies(xt, row_send, row_recv)
    start_up(x_rows)
    start_down(x_rows)
    lax.fori_loop(1, CHUNK, turn, 0, unroll=3)
    for q in order[2:]:
        widen(q)
    if chunks > 1:
        turn(CHUNK, 0)

    def turn_rest():
        if chunks > 1:
            lax.fori_loop(CHUNK + 1, rows - 1, turn, 0, unroll=2)

    loads["w"].wait()

    wf[...] = jnp.zeros(wf.shape, bf16)
    for a in range(3):
        for b in range(3):
            wf[b * padded : b * padded + outputs, a * channels : (a + 1) * channels] = w_ref[a, b]

    lane = lax.broadcasted_iota(jnp.int32, (padded, cols), 1)
    thin = lax.broadcasted_iota(jnp.int32, (CHUNK, cols), 1)

    def forward(pair, q):
        rhs = jnp.concatenate(
            [xt[pl.ds(2 * pair + i, 3)].reshape(3 * channels, cols) for i in range(2)], axis=1)
        y = jnp.dot(wf[...], rhs, preferred_element_type=f32)
        for i in range(2):
            r = 2 * pair + i
            from_left, mid, from_right = [
                y[b * padded : (b + 1) * padded, i * cols : (i + 1) * cols] for b in range(3)]
            from_left = pltpu.roll(from_left, 1, 1)
            from_right = pltpu.roll(from_right, cols - 1, 1)
            slot = r - q * CHUNK
            both = pltpu.roll(jnp.where(lane == 0, from_left, from_right), 2 * slot + 1, 1)
            turned[0, 0:padded, :] = jnp.where(lane // 2 == slot, both, turned[0, 0:padded, :])
            total = mid + jnp.where(lane == 0, 0.0, from_left)
            total = total + jnp.where(lane == cols - 1, 0.0, from_right)
            pf[pl.ds(r, padded, stride=pitch), :] = total

    def edge_copies(q, source, target, send, recv):
        return [
            pltpu.make_async_remote_copy(
                src_ref=source.at[q, s], dst_ref=target.at[q, s], send_sem=send.at[q, s],
                recv_sem=recv.at[q, s], device_id=(me, lat, side), device_id_type=MESH)
            for s, side in enumerate((right, left))]

    def run_pairs(pairs, body):
        pairs = sorted(pairs)
        while pairs:
            n = 1
            while n < len(pairs) and pairs[n] == pairs[0] + n:
                n += 1

            def step(pair, carry):
                body(pair)
                return carry

            lax.fori_loop(pairs[0], pairs[0] + n, step, 0, unroll=math.gcd(n, 2) if n % 2 == 0 else n if n < 8 else 1)
            pairs = pairs[n:]

    peer = lambda q, step: pltpu.make_async_remote_copy(
        src_ref=p_ref.at[:, pl.ds(q * CHUNK, CHUNK), :],
        dst_ref=others.at[step - 1, :, pl.ds(q * CHUNK, CHUNK), :],
        send_sem=peer_send.at[q, step - 1], recv_sem=peer_recv.at[q, step - 1],
        device_id=(lax.rem(me + step, members), lat, lon), device_id_type=MESH)

    edges = {}

    def finish(q):
        for copy in edges[q]:
            copy.wait()

        left_edge, right_edge = edge_in[q, 0], edge_in[q, 1]

        def pack(o, carry):
            at = pl.ds(pl.multiple_of(o * pitch + q * CHUNK, 8), CHUNK)
            total = pf[at, :]
            total = total + jnp.where(thin == 0, pltpu.roll(left_edge, lax.rem(cols - o, cols), 1), 0.0)
            total = total + jnp.where(thin == cols - 1, pltpu.roll(right_edge, cols - 1 - o, 1), 0.0)
            p_ref[o, q * CHUNK : (q + 1) * CHUNK, :] = (total + bias_ref[o]).astype(bf16)
            return carry

        lax.fori_loop(0, outputs, pack, 0, unroll=spread)

        def send(step, carry):
            peer(q, step).start()
            return carry

        lax.fori_loop(1, members, send, 0)

    half = CHUNK // 2
    turned[0] = jnp.zeros(turned.shape[1:], f32)
    waited = False
    for at, q in enumerate(order):
        pairs = range(q * half, (q + 1) * half)
        bounds = [p for p in pairs if p in (0, rows // 2 - 1)]
        run_pairs([p for p in pairs if p not in bounds], lambda p: forward(p, q))
        if bounds and not waited:
            wait_rows(x_rows, xt)
            waited = True
        for p in bounds:
            forward(p, q)
        turned[1] = jnp.transpose(turned[0])
        edge_out[q, 0] = turned[1, pl.ds(1, CHUNK, stride=2), :]
        edge_out[q, 1] = turned[1, pl.ds(0, CHUNK, stride=2), :]
        edges[q] = edge_copies(q, edge_out, edge_in, edge_send, edge_recv)
        for copy in edges[q]:
            copy.start()
        if at == 0:
            turn_rest()
        if at == 0 and len(order) > 1:
            finish(q)
        elif at > 1:
            finish(order[at - 1])
    wbt[...] = jnp.zeros(wbt.shape, bf16)
    for a in range(3):
        for b in range(3):
            base = ((2 - a) * 3 + b) * padded
            wbt[base : base + outputs, :] = w_ref[a, b]
    wb[...] = jnp.transpose(wbt[...])
    row_index = (lat * rows + lax.broadcasted_iota(jnp.int32, (rows, cols), 0)).astype(f32)
    latw[...] = jnp.cos((-80.0 + 160.0 * (row_index + 0.5) / float(rows * lats)) * (jnp.pi / 180.0))

    loads["obs"].wait()

    def misfits(q):
        inside = slice(q * CHUNK, (q + 1) * CHUNK)

        def misfit(o, carry):
            at = pl.ds(pl.multiple_of(o * pitch + q * CHUNK, 8), CHUNK)
            g[at, :] = smooth(p_ref[o, inside, :].astype(f32) - obs_ref[o, inside, :].astype(f32))
            return carry

        lax.fori_loop(0, outputs, misfit, 0, unroll=spread)

    g[pl.ds(outputs * pitch, (padded - outputs) * pitch), :] = jnp.zeros(
        ((padded - outputs) * pitch, cols), f32)
    for q in order[:-1]:
        misfits(q)
    finish(order[-1])
    misfits(order[-1])

    def gradient(q):
        inside = slice(q * CHUNK, (q + 1) * CHUNK)

        def arrive(step, carry):
            peer(q, step).wait()
            return carry

        lax.fori_loop(1, members, arrive, 0)
        weight_row = latw[inside, :]

        def score(o, carry):
            at = pl.ds(pl.multiple_of(o * pitch + q * CHUNK, 8), CHUNK)
            own = p_ref[o, inside, :].astype(f32)
            add = lambda j, run: run + smooth(own - others[j, o, inside, :].astype(f32))
            pair_sum = smooth(own - own)
            if members == 2:
                pair_sum = add(0, pair_sum)
            else:
                pair_sum = lax.fori_loop(0, members - 1, add, pair_sum)
            value = weight_row * var_ref[o] * (g[at, :] - pair_sum / (members - 1))
            value = value.astype(bf16).astype(f32)
            g[at, :] = value
            to_right, to_left = carry
            to_right = jnp.where(thin == o, pltpu.roll(value, o + 1, 1), to_right)
            to_left = jnp.where(thin == o, pltpu.roll(value, o, 1), to_left)
            return to_right, to_left

        zero = jnp.zeros((CHUNK, cols), f32)
        gedge_out[q, 0], gedge_out[q, 1] = lax.fori_loop(
            0, outputs, score, (zero, zero), unroll=spread)
        copies = edge_copies(q, gedge_out, gedge_in, gedge_send, gedge_recv)
        for copy in copies:
            copy.start()
        return copies

    def shifted(q):
        turned[1, pl.ds(0, CHUNK, stride=2), :] = gedge_in[q, 1]
        turned[1, pl.ds(1, CHUNK, stride=2), :] = gedge_in[q, 0]
        turned[0] = jnp.transpose(turned[1])

        def one(r, carry):
            row = g[pl.ds(r, padded, stride=pitch), :]
            both = pltpu.roll(turned[0, 0:padded, :], cols - 1 - 2 * (r - q * CHUNK), 1)
            ahead = jnp.where(lane == cols - 1, both, pltpu.roll(row, cols - 1, 1))
            behind = jnp.where(lane == 0, both, pltpu.roll(row, 1, 1))
            gs[r + 1, 0:padded, :] = ahead.astype(bf16)
            gs[r + 1, padded : 2 * padded, :] = row.astype(bf16)
            gs[r + 1, 2 * padded :, :] = behind.astype(bf16)
            return carry

        lax.fori_loop(q * CHUNK, (q + 1) * CHUNK, one, 0, unroll=4)

    def backward(pair):
        rhs = jnp.concatenate(
            [gs[pl.ds(2 * pair + i, 3)].reshape(9 * padded, cols) for i in range(2)], axis=1)
        y = jnp.dot(wb[:, : 9 * padded], rhs, preferred_element_type=f32)
        for i in range(2):
            big[pl.ds(2 * pair + i, channels, stride=pitch), :] = y[:, i * cols : (i + 1) * cols]

    g_rows = row_copies(gs, grow_send, grow_recv)
    ready, done = set(), set()

    def runnable():
        new = [p for p in range(1, rows // 2 - 1)
               if p not in done and {2 * p - 1, 2 * p, 2 * p + 1, 2 * p + 2} <= ready]
        done.update(new)
        return new

    def settle(q, copies):
        for copy in copies:
            copy.wait()
        shifted(q)
        ready.update(range(q * CHUNK, (q + 1) * CHUNK))
        if q == 0:
            start_up(g_rows)
        if q == chunks - 1:
            start_down(g_rows)

    early = order[:-1]
    moving = [(q, gradient(q)) for q in early]
    for q, copies in moving:
        settle(q, copies)
    work = runnable()
    run_pairs(work[: len(work) // 2], backward)
    last = order[-1]
    copies = gradient(last)
    run_pairs(work[len(work) // 2 :], backward)
    if len(order) > 2:
        wait_rows(g_rows, gs)
        run_pairs([0], backward)
        run_pairs([rows // 2 - 1], backward)
    settle(last, copies)
    run_pairs(runnable(), backward)
    if len(order) <= 2:
        wait_rows(g_rows, gs)
        run_pairs([0], backward)
        run_pairs([rows // 2 - 1], backward)

    def narrow(c, carry):
        start = pl.multiple_of(c * pitch, 8)
        out_ref[c] = big[pl.ds(start, rows), :].astype(bf16)
        return carry

    lax.fori_loop(0, channels, narrow, 0, unroll=8)


def shards(layer_inputs, conv_weight, channel_offset, observed, var_weight):
    _, channels, rows, cols = layer_inputs.shape
    outputs = conv_weight.shape[2]
    members, lats, lons = [lax.axis_size(n) for n in ("member", "lat", "lon")]
    padded = -(-outputs // 16) * 16
    chunks = rows // CHUNK
    sizes = (members, lats, lons, channels, rows, cols, outputs, padded)
    vmem = pl.BlockSpec(memory_space=pltpu.VMEM)
    smem = pl.BlockSpec(memory_space=pltpu.SMEM)
    edge = pltpu.VMEM((chunks, 2, CHUNK, cols), f32)
    hbm = pl.BlockSpec(memory_space=pl.ANY)
    dma = pltpu.SemaphoreType.DMA
    predicted, slope = pl.pallas_call(
        functools.partial(kernel, sizes),
        out_shape=(
            pltpu.VMEM((outputs, rows, cols), bf16),
            pltpu.VMEM((channels, rows, cols), bf16),
        ),
        in_specs=[hbm, hbm, hbm, smem, smem],
        out_specs=(vmem, vmem),
        scratch_shapes=[
            pltpu.VMEM((channels, rows, cols), bf16),
            pltpu.VMEM(conv_weight.shape, bf16),
            pltpu.VMEM((outputs, rows, cols), bf16),
            dma((chunks + 2,)),
            pltpu.VMEM((channels * pitch_of(rows), cols), f32),
            pltpu.VMEM((rows + 2, channels, cols), bf16),
            pltpu.VMEM((3 * padded, 3 * channels), bf16),
            pltpu.VMEM((-(-9 * padded // 128) * 128, channels), bf16),
            pltpu.VMEM((channels, -(-9 * padded // 128) * 128), bf16),
            pltpu.VMEM((padded * pitch_of(rows), cols), f32),
            pltpu.VMEM((padded * pitch_of(rows), cols), f32),
            pltpu.VMEM((rows + 2, 3 * padded, cols), bf16),
            pltpu.VMEM((members - 1, outputs, rows, cols), bf16),
            pltpu.VMEM((rows, cols), f32),
            pltpu.VMEM((2, cols, cols), f32),
            edge, edge, edge, edge,
            dma((2,)), dma((2,)), dma((2,)), dma((2,)),
            dma((chunks, 2)), dma((chunks, 2)), dma((chunks, 2)), dma((chunks, 2)),
            dma((chunks, members - 1)), dma((chunks, members - 1)),
        ],
        compiler_params=pltpu.CompilerParams(
            collective_id=0, has_side_effects=True, vmem_limit_bytes=60 * 1024 * 1024),
        name="crps_step",
    )(layer_inputs[0], conv_weight, observed, channel_offset, var_weight)
    return predicted[None], slope[None]


def solution(mesh):
    in_specs = (P("member", None, "lat", "lon"), P(), P(), P(None, "lat", "lon"), P())
    out_specs = (P("member", None, "lat", "lon"), P("member", None, "lat", "lon"))
    return jax.shard_map(shards, mesh=mesh, in_specs=in_specs, out_specs=out_specs, check_vma=False)
```
